32 devices in a mesh: row: 8 (over z, x), col: 4 (over y, core).
Axes of the slice: x: 2, y: 2, z: 4, core: 2. Of those that a mesh axis runs over, the one named last changes fastest.
Arguments:
- tokens: bfloat16 [64, 12288], P('row', 'col'), may hold values from -6 to 6
- past_tokens: bfloat16 [64, 12288], P('row', 'col'), may hold values from -6 to 6
- out_grad: bfloat16 [64, 12288], P('row', 'col'), may hold values from -3 to 3
- w_in: bfloat16 [12288, 24576], P('col', 'row'), may hold values from -0.0546875 to 0.0546875
- w_out: bfloat16 [24576, 12288], P('row', 'col'), may hold values from -0.0390625 to 0.0390625
Outputs:
- layer_out: bfloat16 [64, 12288], P('row', 'col')
- input_grad: bfloat16 [64, 12288], P('row', 'col')
- grad_w_in: bfloat16 [12288, 24576], P('col', 'row')
- grad_w_out: bfloat16 [24576, 12288], P('row', 'col')
The draws below stay inside these ranges and needn't reach their ends.
All inputs are finite; a program needn't handle non-finite values.
Results may differ from the reference program's by a relative error of at most 0.005.
Values may be sent and summed in bfloat16 or wider, within the bound.
No kernel may reach another device: no remote copies, remote signals or barrier semaphores. Data moves between devices by JAX's collectives and lax.ppermute only.
A program may use at most 128 MiB of HBM per device.

```python
import jax
import jax.numpy as jnp

D = 12288
FF = 24576
TOKENS = 64


def steps_of(rng, extent, pieces, least, high):
    level, own = 1.0, jax.random.fold_in(rng, 6)
    for position, parts in pieces:
        draws = jnp.exp(jax.random.uniform(jax.random.fold_in(own, position), (parts,), jnp.float32, least / len(pieces), high / len(pieces)))
        level = level * jnp.repeat(draws, extent[position] // parts).reshape([-1 if axis == position else 1 for axis in range(len(extent))])
    return level


def centred(own_key, shape, spread, reach, shards=(), kind=jnp.bfloat16):
    result = jax.random.normal(own_key, shape, jnp.float32) * spread
    if len(shards) > 0:
        result = steps_of(own_key, shape, shards, -0.22, 0.18) * result
    return jnp.clip(result, min=-reach, max=reach).astype(kind)


def setup_inputs(seed: int = 0) -> dict:
    streams_of = jax.random.split(jax.random.key(seed), 6)
    tokens = centred(streams_of[0], (TOKENS, D), 1.0, 6.0, ((0, 8), (1, 4)))
    past_tokens = centred(streams_of[1], (TOKENS, D), 1.0, 6.0, ((0, 8), (1, 4)))
    out_grad = centred(streams_of[2], (TOKENS, D), 0.5, 3.0, ((0, 8), (1, 4)))
    w_in = centred(streams_of[3], (D, FF), D ** -0.5, 0.0546875, ((0, 4), (1, 8)))
    w_out = centred(streams_of[4], (FF, D), FF ** -0.5, 0.0390625, ((0, 8), (1, 4)))
    return {"tokens": tokens, "past_tokens": past_tokens, "out_grad": out_grad, "w_in": w_in, "w_out": w_out}


def gelu_parts(pre):
    cdf = 0.5 * (1.0 + jax.scipy.special.erf(pre * 0.7071067811865476))
    slope = cdf + pre * jnp.exp(-0.5 * pre * pre) * 0.3989422804014327
    return pre * cdf, slope


def reference(tokens, past_tokens, out_grad, w_in, w_out):
    pre = jnp.dot(tokens, w_in, preferred_element_type=jnp.float32)
    hidden = gelu_parts(pre)[0].astype(jnp.bfloat16)
    layer_out = jnp.dot(hidden, w_out, preferred_element_type=jnp.float32).astype(jnp.bfloat16)
    past_pre = jnp.dot(past_tokens, w_in, preferred_element_type=jnp.float32)
    past_act, slope = gelu_parts(past_pre)
    past_hidden = past_act.astype(jnp.bfloat16)
    back = jnp.dot(out_grad, w_out.T, preferred_element_type=jnp.float32)
    hidden_grad = (back * slope).astype(jnp.bfloat16)
    grad_w_out = jnp.dot(past_hidden.T, out_grad, preferred_element_type=jnp.float32).astype(jnp.bfloat16)
    grad_w_in = jnp.dot(past_tokens.T, hidden_grad, preferred_element_type=jnp.float32).astype(jnp.bfloat16)
    input_grad = jnp.dot(hidden_grad, w_in.T, preferred_element_type=jnp.float32).astype(jnp.bfloat16)
    return layer_out, input_grad, grad_w_in, grad_w_out
```

```python
import jax
import jax.numpy as jnp
from jax import lax
from jax.sharding import PartitionSpec as P

BF16, F32 = jnp.bfloat16, jnp.float32


def gelu_parts(pre):
    cdf = 0.5 * (1.0 + jax.scipy.special.erf(pre * 0.7071067811865476))
    slope = cdf + pre * jnp.exp(-0.5 * pre * pre) * 0.3989422804014327
    return (pre * cdf, slope)


def swap(x, axis, bit):
    n = lax.axis_size(axis)
    return lax.ppermute(x, axis, [(i, i ^ bit) for i in range(n)])


def bits(n):
    return [1 << k for k in range(n.bit_length() - 1)]


def gather(x, axis, dim):
    for bit in reversed(bits(lax.axis_size(axis))):
        x = jnp.concatenate([x, swap(x, axis, bit)], axis=dim)
    return x


def scatter(x):
    for bit in bits(lax.axis_size("row")):
        half = x.shape[0] // 2
        got = swap(x[half:].astype(BF16), "row", bit)
        x = x[:half] + got.astype(F32)
    return x


def total(x):
    me = lax.axis_index("col")
    half = x.shape[1] // 2
    keep = (me % 2) * half
    mine = lax.dynamic_slice_in_dim(x, keep, half, 1)
    other = lax.dynamic_slice_in_dim(x, half - keep, half, 1)
    x = mine + swap(other, "col", 1)
    for bit in bits(lax.axis_size("col"))[1:]:
        x = x + swap(x.astype(BF16), "col", bit).astype(F32)
    return x


def whole(x):
    other = swap(x, "col", 1)
    low = lax.axis_index("col") % 2 == 0
    return jnp.concatenate([jnp.where(low, x, other), jnp.where(low, other, x)], axis=1)


def local(tokens, past_tokens, out_grad, w_in, w_out):
    x = gather(jnp.stack([tokens, past_tokens, out_grad]), "row", 1)
    both, grad_all = x[:2], x[2]
    past_all = x[1]
    n = both.shape[1]
    back = lax.dot_general(grad_all, w_out, (((1,), (1,)), ((), ())), preferred_element_type=F32)
    pre = jnp.dot(both.reshape(2 * n, -1), w_in, preferred_element_type=F32).reshape(2, n, -1)
    s = total(jnp.concatenate([pre, back[None]]))
    hidden = gelu_parts(s[0])[0]
    act, slope = gelu_parts(s[1])
    h = whole(jnp.stack([hidden, act, s[2] * slope]).astype(BF16))
    hidden_all, act_all, hidden_grad = h[0], h[1], h[2]
    layer = jnp.dot(hidden_all, w_out, preferred_element_type=F32)
    inp = lax.dot_general(hidden_grad, w_in, (((1,), (1,)), ((), ())), preferred_element_type=F32)
    res = scatter(jnp.concatenate([layer, inp], axis=1)).astype(BF16)
    width = layer.shape[1]
    grad_w_out = lax.dot_general(
        act_all, grad_all, (((0,), (0,)), ((), ())), preferred_element_type=F32
    ).astype(BF16)
    grad_w_in = lax.dot_general(
        past_all, hidden_grad, (((0,), (0,)), ((), ())), preferred_element_type=F32
    ).astype(BF16)
    return (res[:, :width], res[:, width:], grad_w_in, grad_w_out)


def solution(mesh):
    in_specs = (P("row", "col"), P("row", "col"), P("row", "col"), P("col", "row"), P("row", "col"))
    out_specs = (P("row", "col"), P("row", "col"), P("col", "row"), P("row", "col"))
    return jax.shard_map(local, mesh=mesh, in_specs=in_specs, out_specs=out_specs, check_vma=False)
```

```python
import jax
import jax.numpy as jnp
from jax import lax
from jax.experimental import pallas as pl
from jax.experimental.pallas import tpu as pltpu
from jax.sharding import PartitionSpec as P


BF16, F32 = jnp.bfloat16, jnp.float32
MIB = 1 << 20
FLOPS = 128
NN, NT, TN = ((1,), (0,)), ((1,), (1,)), ((0,), (0,))


def gelu_parts(pre):
    cdf = 0.5 * (1.0 + jax.scipy.special.erf(pre * 0.7071067811865476))
    slope = cdf + pre * jnp.exp(-0.5 * pre * pre) * 0.3989422804014327
    return (pre * cdf, slope)


def swap(x, axis, bit):
    n = lax.axis_size(axis)
    return lax.ppermute(x, axis, [(i, i ^ bit) for i in range(n)])


def bits(n):
    return [1 << k for k in range(n.bit_length() - 1)]


def block_of(n, most):
    return max(b for b in range(128, n + 1, 128) if n % b == 0 and b <= max(most, 128))


def dot(x, y, dims):
    return lax.dot_general(x, y, (dims, ((), ())), preferred_element_type=F32)


def call(kernel, in_specs, out_specs, out_shape, scratch, macs, moved, *args, grant=6, aliases={}, after=None):
    body = kernel
    if after is not None:
        in_specs, args = [*in_specs, pl.BlockSpec(memory_space=pl.ANY)], (*args, after)
        at = len(args) - 1

        def body(*refs):
            kernel(*refs[:at], *refs[at + 1 :])

    return pl.pallas_call(
        body,
        in_specs=in_specs,
        out_specs=out_specs,
        out_shape=out_shape,
        scratch_shapes=scratch,
        input_output_aliases=aliases,
        compiler_params=pltpu.CompilerParams(vmem_limit_bytes=grant * MIB),
        cost_estimate=pl.CostEstimate(flops=FLOPS * macs, bytes_accessed=moved, transcendentals=0),
    )(*args)


VMEM = pl.BlockSpec(memory_space=pltpu.VMEM)
SMEM = pl.BlockSpec(memory_space=pltpu.SMEM)
HBM = pl.BlockSpec(memory_space=pltpu.HBM)


def core():
    return lax.rem(lax.axis_index("col"), 2)


def load(w, after, parts=8):
    rows = w.shape[0] // parts

    def kernel(w_ref, o_ref, sems):
        copies = [
            pltpu.make_async_copy(w_ref.at[pl.ds(i * rows, rows)], o_ref.at[pl.ds(i * rows, rows)], sems.at[i])
            for i in range(parts)
        ]
        for copy in copies:
            copy.start()
        for copy in copies:
            copy.wait()

    return call(
        kernel,
        [HBM],
        VMEM,
        pltpu.VMEM(w.shape, w.dtype),
        [pltpu.SemaphoreType.DMA((parts,))],
        w.size,
        2 * w.size,
        pltpu.with_memory_space_constraint(w, pltpu.HBM),
        grant=2,
        after=after,
    )


def stream(w_ref, held, sems, b, free, body, ahead=3):
    n = w_ref.shape[free] // b

    def part(j):
        return pl.ds(pl.multiple_of(j * b, b), b)

    def copy(j):
        at = (slice(None), part(j)) if free == 1 else (part(j), slice(None))
        return pltpu.make_async_copy(w_ref.at[at], held.at[at], sems.at[j])

    if sems is not None:
        for j in range(min(ahead, n)):
            copy(j).start()

    @pl.loop(0, n)
    def _(j):
        if sems is not None:
            copy(j).wait()

            @pl.when(j + ahead < n)
            def _():
                copy(j + ahead).start()

        body(part(j))


def into(x, y, w, rows, dims, after=None):
    free = 1 - dims[1][0]
    k, n = w.shape[dims[1][0]], w.shape[free]
    h = x.shape[1]
    first, count, groups = rows
    tall = count // groups // 2
    here = after is None
    b = block_of(n, 1024 if here else 512)

    def kernel(core_ref, x_ref, y_ref, w_ref, mine_ref, send_ref, held, *sems):
        one = pl.ds(first, count)
        low = core_ref[0] == 0
        w_from = w_ref if here else held

        def body(part):
            if free == 1:
                left, right = w_from[:h, part], w_from[h:, part]
            else:
                left, right = w_from[part, :h], w_from[part, h:]
            acc = dot(x_ref[one, :], left, dims) + dot(y_ref[one, :], right, dims)
            for g in range(groups):
                at = 2 * g * tall
                lo, hi = acc[at : at + tall], acc[at + tall : at + 2 * tall]
                put = pl.ds(g * tall, tall)
                mine_ref[put, part] = jnp.where(low, lo, hi)
                send_ref[put, part] = jnp.where(low, hi, lo)

        stream(w_ref, held, None if here else sems[0], b, free, body)

    shape = jax.ShapeDtypeStruct((count // 2, n), F32)
    me = jnp.full((1,), core(), jnp.int32)
    space = pltpu.VMEM if here else pltpu.HBM
    return call(
        kernel,
        [SMEM, VMEM, VMEM, VMEM if here else HBM],
        [VMEM, VMEM, VMEM],
        [shape, shape, pltpu.VMEM(w.shape, w.dtype)],
        [] if here else [pltpu.SemaphoreType.DMA((n // b,))],
        k * n,
        2 * k * n,
        me,
        x,
        y,
        pltpu.with_memory_space_constraint(w, space),
        aliases={3: 2} if here else {},
        after=after,
    )


def outof(own, other, w, dims, here, after):
    free = 1 - dims[1][0]
    k, n = w.shape[dims[1][0]], w.shape[free]
    half = own.shape[0]
    b = block_of(n, 1024 if here else 512)

    def kernel(core_ref, own_ref, other_ref, w_ref, keep_ref, send_ref, x_ref, *scratch):
        low = core_ref[0] == 0
        one, two = own_ref[...], other_ref[...]
        x_ref[:half, :] = jnp.where(low, one, two)
        x_ref[half:, :] = jnp.where(low, two, one)
        held, sems = scratch or (w_ref, None)

        def body(part):
            acc = dot(x_ref[...], held[:, part] if free == 1 else held[part, :], dims)
            keep_ref[:, part] = acc[:half]
            send_ref[:, part] = acc[half:].astype(BF16)

        stream(w_ref, held, sems, b, free, body)

    me = jnp.full((1,), core(), jnp.int32)
    scratch = [] if here else [pltpu.VMEM(w.shape, w.dtype), pltpu.SemaphoreType.DMA((n // b,))]
    return call(
        kernel,
        [SMEM, VMEM, VMEM, VMEM if here else HBM],
        [VMEM, VMEM],
        [jax.ShapeDtypeStruct((half, n), F32), jax.ShapeDtypeStruct((half, n), BF16)],
        [pltpu.VMEM((2 * half, k), BF16), *scratch],
        k * n,
        2 * k * n,
        me,
        own,
        other,
        pltpu.with_memory_space_constraint(w, pltpu.VMEM if here else pltpu.HBM),
        grant=6 if here else 26,
        after=after,
    )


def outer(jobs, after):
    blocks, olds = [], []
    for i, (x, _, old, first, rows) in enumerate(jobs):
        b = block_of(rows, 512)
        blocks += [(i, first + j, b) for j in range(0, rows, b)]
        if old is not None:
            olds.append((i, pltpu.with_memory_space_constraint(old, pltpu.HBM)))
    tall = max(b for _, _, b in blocks)
    width = jobs[0][1].shape[1]
    count = len(jobs)

    def kernel(*refs):
        sides = refs[: 2 * count]
        outs = refs[2 * count + len(olds) : 3 * count + len(olds)]
        held, sems = refs[3 * count + len(olds) :]
        copies = []
        for at, (i, row, b) in enumerate(blocks):
            part = pl.ds(row, b)
            space = held.at[at, pl.ds(0, b)]
            space[...] = dot(sides[2 * i][:, part], sides[2 * i + 1][...], TN).astype(BF16)
            copies.append(pltpu.make_async_copy(space, outs[i].at[part], sems.at[at]))
            copies[-1].start()
        for copy in copies:
            copy.wait()

    moved = sum(b for _, _, b in blocks) * width
    return call(
        kernel,
        [VMEM] * (2 * count) + [HBM] * len(olds),
        [HBM] * count,
        [pltpu.HBM((x.shape[1], width), BF16) for x, *_ in jobs],
        [pltpu.VMEM((len(blocks), tall, width), BF16), pltpu.SemaphoreType.DMA((len(blocks),))],
        moved,
        2 * moved,
        *[side for x, y, *_ in jobs for side in (x, y)],
        *[old for _, old in olds],
        grant=20,
        aliases={2 * count + at: i for at, (i, _) in enumerate(olds)},
        after=after,
    )


def gather(left, right):
    all_bits = bits(lax.axis_size("row"))
    one = all_bits[::-1]
    two = all_bits[:1] + all_bits[:0:-1]
    order_one, order_two = [0], [0]
    tall = left.shape[1]
    for a, b in zip(one, two):
        last = right
        from_left, from_right = swap(left, "row", a), swap(right, "row", b)
        left = jnp.concatenate([left, from_left], axis=1)
        right = jnp.concatenate([right, from_right], axis=1)
        order_one += [j ^ a for j in order_one]
        order_two += [j ^ b for j in order_two]
    at = [order_two.index(j) * tall for j in order_one]
    right = jnp.concatenate([right[:, i : i + tall] for i in at], axis=1)
    return left, right, last


def pair_sum(mine, send):
    return mine + swap(send, "col", 1)


def col_send(x):
    return lax.optimization_barrier(x.astype(BF16))


def col_sum(x, sent):
    for bit in bits(lax.axis_size("col"))[1:]:
        x = x + swap(sent, "col", bit).astype(F32)
        sent = x.astype(BF16)
    return x


def in_order(own, other):
    low = core() == 0
    return jnp.concatenate([jnp.where(low, own, other), jnp.where(low, other, own)], axis=0)


def local(tokens, past_tokens, out_grad, w_in, w_out):
    x = lax.optimization_barrier(jnp.stack([tokens, past_tokens, out_grad]))
    width = x.shape[2]
    h = width // 2
    left, right, last = gather(x[:, :, :h], x[:, :, h:])
    n = left.shape[1]
    half = n // 2
    left, right = left.reshape(3 * n, h), right.reshape(3 * n, h)
    mine, send, w_in_here = into(left, right, load(w_in, last), (0, 2 * n, 2), NN)
    pre = pair_sum(mine, send)
    pre_sent = col_send(pre)
    mine, send, w_out_here = into(left, right, w_out, (2 * n, n, 1), NT, pre_sent)
    back = pair_sum(mine, send)
    back_sent = col_send(back)
    pre = col_sum(pre, pre_sent)
    hidden = gelu_parts(pre[:half])[0]
    act, slope = gelu_parts(pre[half:])
    own, slope = lax.optimization_barrier((jnp.concatenate([hidden, act], axis=0).astype(BF16), slope))
    other = swap(own, "col", 1)
    layer = outof(own[:half], other[:half], w_out_here, NN, True, back_sent)
    back = col_sum(back, back_sent)
    own_grad = (back * slope).astype(BF16)
    other_grad = swap(own_grad, "col", 1)
    inp = outof(own_grad, other_grad, w_in_here, NT, True, layer[1])
    past_all = jnp.concatenate([left[n : 2 * n], right[n : 2 * n]], axis=1)
    grad_all = jnp.concatenate([left[2 * n :], right[2 * n :]], axis=1)
    row_bits = bits(lax.axis_size("row"))
    sums = [keep + swap(send, "row", row_bits[0]).astype(F32) for (keep, send) in (layer, inp)]
    act_all, hidden_grad = in_order(own[half:], other[half:]), in_order(own_grad, other_grad)
    units = act_all.shape[1], past_all.shape[1]
    share = units[0] * 2 // 3 // 128 * 128, units[1] // 3 // 128 * 128
    (grad_w_out,) = outer([(act_all, grad_all, None, 0, share[0])], inp[1])
    res = jnp.concatenate(sums, axis=1)
    for i, bit in enumerate(row_bits[1:]):
        m = res.shape[0] // 2
        sent = lax.optimization_barrier(res[m:].astype(BF16))
        if i == 0:
            grad_w_out, grad_w_in = outer(
                [
                    (act_all, grad_all, grad_w_out, share[0], units[0] - share[0]),
                    (past_all, hidden_grad, None, 0, share[1]),
                ],
                sent,
            )
        elif i == 1:
            (grad_w_in,) = outer([(past_all, hidden_grad, grad_w_in, share[1], units[1] - share[1])], sent)
        res = res[:m] + swap(sent, "row", bit).astype(F32)
    res = res.astype(BF16)
    return (res[:, :width], res[:, width:], grad_w_in, grad_w_out)


def solution(mesh):
    in_specs = (P("row", "col"), P("row", "col"), P("row", "col"), P("col", "row"), P("row", "col"))
    out_specs = (P("row", "col"), P("row", "col"), P("col", "row"), P("row", "col"))

    return jax.shard_map(local, mesh=mesh, in_specs=in_specs, out_specs=out_specs, check_vma=False)
```

```python
import jax
import jax.numpy as jnp
from jax import lax
from jax.experimental import pallas as pl
from jax.experimental.pallas import tpu as pltpu
from jax.sharding import PartitionSpec as P


BF16, F32 = jnp.bfloat16, jnp.float32
MIB = 1 << 20
FLOPS = 128
NN, NT = ((1,), (0,)), ((1,), (1,))


def gelu_parts(pre):
    cdf = 0.5 * (1.0 + jax.scipy.special.erf(pre * 0.7071067811865476))
    slope = cdf + pre * jnp.exp(-0.5 * pre * pre) * 0.3989422804014327
    return (pre * cdf, slope)


def swap(x, axis, bit):
    n = lax.axis_size(axis)
    return lax.ppermute(x, axis, [(i, i ^ bit) for i in range(n)])


def bits(n):
    return [1 << k for k in range(n.bit_length() - 1)]


def block_of(n, most):
    return max(b for b in range(128, n + 1, 128) if n % b == 0 and b <= max(most, 128))


def dot(x, y, dims):
    return lax.dot_general(x, y, (dims, ((), ())), preferred_element_type=F32)


def call(kernel, in_specs, out_specs, out_shape, scratch, macs, moved, *args, grant=6, aliases={}, after=None):
    body = kernel
    if after is not None:
        in_specs, args = [*in_specs, pl.BlockSpec(memory_space=pl.ANY)], (*args, after)
        at = len(args) - 1

        def body(*refs):
            kernel(*refs[:at], *refs[at + 1 :])

    return pl.pallas_call(
        body,
        in_specs=in_specs,
        out_specs=out_specs,
        out_shape=out_shape,
        scratch_shapes=scratch,
        input_output_aliases=aliases,
        compiler_params=pltpu.CompilerParams(vmem_limit_bytes=grant * MIB),
        cost_estimate=pl.CostEstimate(flops=FLOPS * macs, bytes_accessed=moved, transcendentals=0),
    )(*args)


VMEM = pl.BlockSpec(memory_space=pltpu.VMEM)
SMEM = pl.BlockSpec(memory_space=pltpu.SMEM)
HBM = pl.BlockSpec(memory_space=pltpu.HBM)


def load(w, held, first, rows, after, parts=4):
    step = rows // parts
    old = [] if held is None else [pltpu.with_memory_space_constraint(held, pltpu.VMEM)]

    def kernel(w_ref, *refs):
        o_ref, sems = refs[-2:]
        copies = []
        for i in range(parts):
            part = pl.ds(first + i * step, step)
            copies.append(pltpu.make_async_copy(w_ref.at[part], o_ref.at[part], sems.at[i]))
            copies[-1].start()
        for copy in copies:
            copy.wait()

    return call(
        kernel,
        [HBM] + [VMEM] * len(old),
        VMEM,
        pltpu.VMEM(w.shape, w.dtype),
        [pltpu.SemaphoreType.DMA((parts,))],
        rows * w.shape[1],
        2 * rows * w.shape[1],
        pltpu.with_memory_space_constraint(w, pltpu.HBM),
        *old,
        grant=2,
        aliases={1: 0} if old else {},
        after=after,
    )


def stream(w_ref, held, sems, b, free, body, ahead=3):
    n = w_ref.shape[free] // b

    def part(j):
        return pl.ds(pl.multiple_of(j * b, b), b)

    def copy(j):
        at = (slice(None), part(j)) if free == 1 else (part(j), slice(None))
        return pltpu.make_async_copy(w_ref.at[at], held.at[at], sems.at[j])

    if sems is not None:
        for j in range(min(ahead, n)):
            copy(j).start()

    @pl.loop(0, n)
    def _(j):
        if sems is not None:
            copy(j).wait()

            @pl.when(j + ahead < n)
            def _():
                copy(j + ahead).start()

        body(part(j))


def into(me, x, y, w, rows, dims, here, sends, after=None):
    free = 1 - dims[1][0]
    k, n = w.shape[dims[1][0]], w.shape[free]
    h = x.shape[1]
    first, count, groups = rows
    tall = count // groups // 2
    b = block_of(n, 1024 if here else 512)

    def kernel(core_ref, x_ref, y_ref, w_ref, mine_ref, send_ref, held, *sems):
        one = pl.ds(first, count)
        low = core_ref[0] == 0
        w_from = w_ref if here else held

        def body(part):
            if free == 1:
                left, right = w_from[:h, part], w_from[h:, part]
            else:
                left, right = w_from[part, :h], w_from[part, h:]
            if free == 1:
                acc = dot(x_ref[one, :], left, NN) + dot(y_ref[one, :], right, NN)
            else:
                acc = (dot(left, x_ref[one, :], NT) + dot(right, y_ref[one, :], NT)).T
            for g in range(groups):
                at = 2 * g * tall
                lo, hi = acc[at : at + tall], acc[at + tall : at + 2 * tall]
                put = pl.ds(g * tall, tall)
                mine_ref[put, part] = jnp.where(low, lo, hi)
                send_ref[put, part] = jnp.where(low, hi, lo).astype(sends)

        stream(w_ref, held, None if here else sems[0], b, free, body)

    half = count // 2, n
    space = pltpu.VMEM if here else pltpu.HBM
    return call(
        kernel,
        [SMEM, VMEM, VMEM, VMEM if here else HBM],
        [VMEM, VMEM, VMEM],
        [jax.ShapeDtypeStruct(half, F32), jax.ShapeDtypeStruct(half, sends), pltpu.VMEM(w.shape, w.dtype)],
        [] if here else [pltpu.SemaphoreType.DMA((n // b,))],
        k * n,
        2 * k * n,
        me,
        x,
        y,
        pltpu.with_memory_space_constraint(w, space),
        aliases={3: 2} if here else {},
        after=after,
    )


def outof(me, own, other, w, dims, here, after):
    free = 1 - dims[1][0]
    k, n = w.shape[dims[1][0]], w.shape[free]
    half = own.shape[0]
    tall = max(2 * half, 128 if free == 1 else 0)
    b = block_of(n, 1024 if here else 512)

    def kernel(core_ref, own_ref, other_ref, w_ref, keep_ref, send_ref, x_ref, *scratch):
        low = core_ref[0] == 0
        one, two = own_ref[...], other_ref[...]
        x_ref[:half, :] = jnp.where(low, one, two)
        x_ref[half : 2 * half, :] = jnp.where(low, two, one)
        if tall > 2 * half:
            x_ref[2 * half :, :] = jnp.zeros((tall - 2 * half, k), BF16)
        held, sems = scratch or (w_ref, None)

        def body(part):
            if free == 1:
                acc = dot(x_ref[...], held[:, part], NN)
            else:
                acc = dot(held[part, :], x_ref[...], NT).T
            keep_ref[:, part] = acc[:half]
            send_ref[:, part] = acc[half : 2 * half].astype(BF16)

        stream(w_ref, held, sems, b, free, body)

    scratch = [] if here else [pltpu.VMEM(w.shape, w.dtype), pltpu.SemaphoreType.DMA((n // b,))]
    return call(
        kernel,
        [SMEM, VMEM, VMEM, VMEM if here else HBM],
        [VMEM, VMEM],
        [jax.ShapeDtypeStruct((half, n), F32), jax.ShapeDtypeStruct((half, n), BF16)],
        [pltpu.VMEM((tall, k), BF16), *scratch],
        k * n,
        2 * k * n,
        me,
        own,
        other,
        pltpu.with_memory_space_constraint(w, pltpu.VMEM if here else pltpu.HBM),
        grant=6 if here else 26,
        after=after,
    )


def outer(jobs, after):
    blocks, olds = [], []
    for i, (x, _, old, first, rows) in enumerate(jobs):
        b = block_of(rows, 1024)
        blocks += [(i, first + j, b) for j in range(0, rows, b)]
        if old is not None:
            olds.append((i, pltpu.with_memory_space_constraint(old, pltpu.HBM)))
    tall = max(b for _, _, b in blocks)
    depth, width = jobs[0][1].shape
    count = len(jobs)
    sizes = [width]
    while len(sizes) < 4 and sizes[-1] % 256 == 0:
        sizes[-1:] = [sizes[-1] // 2] * 2
    cuts = [sizes[::-1]] + [sizes[:1] + [width - sizes[0]]] * (len(blocks) - 2) + [sizes]
    columns = [[(sum(cut[:i]), n) for i, n in enumerate(cut) if n] for cut in cuts[-len(blocks) :]]

    def kernel(*refs):
        sides = refs[: 2 * count]
        outs = refs[2 * count + len(olds) : 3 * count + len(olds)]
        held, turned, sems = refs[3 * count + len(olds) :]
        copies = []
        for at, (i, row, b) in enumerate(blocks):
            part = pl.ds(row, b)
            turned[at, :b, :] = sides[2 * i][:, part].T
            for c, n in columns[at]:
                here = pl.ds(c, n)
                held[at, :b, here] = dot(turned[at, :b, :], sides[2 * i + 1][:, here], NN).astype(BF16)
                copies.append(
                    pltpu.make_async_copy(held.at[at, pl.ds(0, b), here], outs[i].at[part, here], sems.at[len(copies)])
                )
                copies[-1].start()
        for copy in copies:
            copy.wait()

    moved = sum(b for _, _, b in blocks) * width
    return call(
        kernel,
        [VMEM] * (2 * count) + [HBM] * len(olds),
        [HBM] * count,
        [pltpu.HBM((x.shape[1], width), BF16) for x, *_ in jobs],
        [
            pltpu.VMEM((len(blocks), tall, width), BF16),
            pltpu.VMEM((len(blocks), tall, depth), BF16),
            pltpu.SemaphoreType.DMA((sum(len(c) for c in columns),)),
        ],
        moved,
        2 * moved,
        *[side for x, y, *_ in jobs for side in (x, y)],
        *[old for _, old in olds],
        grant=20,
        aliases={2 * count + at: i for at, (i, _) in enumerate(olds)},
        after=after,
    )


def gather(left, right):
    all_bits = bits(lax.axis_size("row"))
    one = all_bits[::-1]
    two = all_bits[:1] + all_bits[:0:-1]
    order_one, order_two, ready = [0], [0], []
    tall = left.shape[1]
    for a, b in zip(one, two):
        ready.append(right)
        from_left, from_right = swap(left, "row", a), swap(right, "row", b)
        left = jnp.concatenate([left, from_left], axis=1)
        right = jnp.concatenate([right, from_right], axis=1)
        order_one += [j ^ a for j in order_one]
        order_two += [j ^ b for j in order_two]
    at = [order_two.index(j) * tall for j in order_one]
    right = jnp.concatenate([right[:, i : i + tall] for i in at], axis=1)
    return left, right, ready


def pair_sum(mine, send):
    return mine + swap(send, "col", 1).astype(F32)


def col_send(x):
    return lax.optimization_barrier(x.astype(BF16))


def col_sum(x, sent):
    for bit in bits(lax.axis_size("col"))[1:]:
        x = x + swap(sent, "col", bit).astype(F32)
        sent = x.astype(BF16)
    return x


def in_order(low, own, other):
    return jnp.concatenate([jnp.where(low, own, other), jnp.where(low, other, own)], axis=0)


def local(tokens, past_tokens, out_grad, w_in, w_out):
    me = lax.rem(lax.axis_index("col"), 2)
    x = jnp.stack([tokens, past_tokens, out_grad])
    x, me, low = lax.optimization_barrier((x, me.reshape(1), me == 0))
    width = x.shape[2]
    h = width // 2
    left, right, ready = gather(x[:, :, :h], x[:, :, h:])
    n = left.shape[1]
    half = n // 2
    left, right = left.reshape(3 * n, h), right.reshape(3 * n, h)
    w_in_here = load(w_in, None, 0, w_in.shape[0], ready[-1], 8)
    part = w_out.shape[0] // 2
    w_out_here = load(w_out, None, 0, part, ready[-3])
    w_out_here = load(w_out, w_out_here, part, part, ready[-2])
    mine, send, w_in_here = into(me, left, right, w_in_here, (0, 2 * n, 2), NN, True, BF16)
    pre = pair_sum(mine, send)
    sent = lax.optimization_barrier((pre[:half].astype(BF16), pre[half:].astype(BF16)))
    mine, send, w_out_here = into(me, left, right, w_out_here, (2 * n, n, 1), NT, True, F32, sent[0])
    back = pair_sum(mine, send)
    back_sent = col_send(back)
    past = col_sum(pre[half:], sent[1])
    act, slope = gelu_parts(past)
    act, slope = lax.optimization_barrier((act.astype(BF16), slope))
    now = col_sum(pre[:half], sent[0])
    hidden = gelu_parts(now)[0].astype(BF16)
    own, slope = lax.optimization_barrier((jnp.concatenate([hidden, act], axis=0), slope))
    other = swap(own, "col", 1)
    layer = outof(me, own[:half], other[:half], w_out_here, NN, True, back_sent)
    back = col_sum(back, back_sent)
    own_grad = (back * slope).astype(BF16)
    other_grad = swap(own_grad, "col", 1)
    inp = outof(me, own_grad, other_grad, w_in_here, NT, True, layer[1])
    past_all = jnp.concatenate([left[n : 2 * n], right[n : 2 * n]], axis=1)
    grad_all = jnp.concatenate([left[2 * n :], right[2 * n :]], axis=1)
    row_bits = bits(lax.axis_size("row"))
    sums = [keep + swap(send, "row", row_bits[0]).astype(F32) for (keep, send) in (layer, inp)]
    act_all, hidden_grad = in_order(low, own[half:], other[half:]), in_order(low, own_grad, other_grad)
    units = act_all.shape[1], past_all.shape[1]
    share = units[0] * 2 // 3 // 128 * 128, units[1] // 3 // 128 * 128
    (grad_w_out,) = outer([(act_all, grad_all, None, 0, share[0])], inp[1])
    res = jnp.concatenate(sums, axis=1)
    for i, bit in enumerate(row_bits[1:]):
        m = res.shape[0] // 2
        sent = lax.optimization_barrier(res[m:].astype(BF16))
        if i == 0:
            grad_w_out, grad_w_in = outer(
                [
                    (act_all, grad_all, grad_w_out, share[0], units[0] - share[0]),
                    (past_all, hidden_grad, None, 0, share[1]),
                ],
                sent,
            )
        elif i == 1:
            (grad_w_in,) = outer([(past_all, hidden_grad, grad_w_in, share[1], units[1] - share[1])], sent)
        res = res[:m] + swap(sent, "row", bit).astype(F32)
    res = res.astype(BF16)
    return (res[:, :width], res[:, width:], grad_w_in, grad_w_out)


def solution(mesh):
    in_specs = (P("row", "col"), P("row", "col"), P("row", "col"), P("col", "row"), P("row", "col"))
    out_specs = (P("row", "col"), P("row", "col"), P("col", "row"), P("row", "col"))

    return jax.shard_map(local, mesh=mesh, in_specs=in_specs, out_specs=out_specs, check_vma=False)
```

```python
import jax
import jax.numpy as jnp
from jax import lax
from jax.experimental import pallas as pl
from jax.experimental.pallas import tpu as pltpu
from jax.sharding import PartitionSpec as P


BF16, F32 = jnp.bfloat16, jnp.float32
MIB = 1 << 20
FLOPS = 128
NN, NT = ((1,), (0,)), ((1,), (1,))


def gelu_parts(pre):
    cdf = 0.5 * (1.0 + jax.scipy.special.erf(pre * 0.7071067811865476))
    slope = cdf + pre * jnp.exp(-0.5 * pre * pre) * 0.3989422804014327
    return (pre * cdf, slope)


def swap(x, axis, bit):
    n = lax.axis_size(axis)
    return lax.ppermute(x, axis, [(i, i ^ bit) for i in range(n)])


def bits(n):
    return [1 << k for k in range(n.bit_length() - 1)]


def block_of(n, most):
    return max(b for b in range(128, n + 1, 128) if n % b == 0 and b <= max(most, 128))


def dot(x, y, dims):
    return lax.dot_general(x, y, (dims, ((), ())), preferred_element_type=F32)


def call(kernel, in_specs, out_specs, out_shape, scratch, macs, moved, *args, grant=6, aliases={}, after=None):
    body = kernel
    if after is not None:
        in_specs, args = [*in_specs, pl.BlockSpec(memory_space=pl.ANY)], (*args, after)
        at = len(args) - 1

        def body(*refs):
            kernel(*refs[:at], *refs[at + 1 :])

    return pl.pallas_call(
        body,
        in_specs=in_specs,
        out_specs=out_specs,
        out_shape=out_shape,
        scratch_shapes=scratch,
        input_output_aliases=aliases,
        compiler_params=pltpu.CompilerParams(vmem_limit_bytes=grant * MIB),
        cost_estimate=pl.CostEstimate(flops=FLOPS * macs, bytes_accessed=moved, transcendentals=0),
    )(*args)


VMEM = pl.BlockSpec(memory_space=pltpu.VMEM)
SMEM = pl.BlockSpec(memory_space=pltpu.SMEM)
HBM = pl.BlockSpec(memory_space=pltpu.HBM)


def load(w, held, first, rows, after, parts=4):
    step = rows // parts
    old = [] if held is None else [pltpu.with_memory_space_constraint(held, pltpu.VMEM)]

    def kernel(w_ref, *refs):
        o_ref, sems = refs[-2:]
        copies = []
        for i in range(parts):
            part = pl.ds(first + i * step, step)
            copies.append(pltpu.make_async_copy(w_ref.at[part], o_ref.at[part], sems.at[i]))
            copies[-1].start()
        for copy in copies:
            copy.wait()

    return call(
        kernel,
        [HBM] + [VMEM] * len(old),
        VMEM,
        pltpu.VMEM(w.shape, w.dtype),
        [pltpu.SemaphoreType.DMA((parts,))],
        rows * w.shape[1],
        2 * rows * w.shape[1],
        pltpu.with_memory_space_constraint(w, pltpu.HBM),
        *old,
        grant=2,
        aliases={1: 0} if old else {},
        after=after,
    )


def stream(w_ref, held, sems, b, free, body, ahead=3):
    n = w_ref.shape[free] // b

    def part(j):
        return pl.ds(pl.multiple_of(j * b, b), b)

    def copy(j):
        at = (slice(None), part(j)) if free == 1 else (part(j), slice(None))
        return pltpu.make_async_copy(w_ref.at[at], held.at[at], sems.at[j])

    if sems is not None:
        for j in range(min(ahead, n)):
            copy(j).start()

    @pl.loop(0, n)
    def _(j):
        if sems is not None:
            copy(j).wait()

            @pl.when(j + ahead < n)
            def _():
                copy(j + ahead).start()

        body(part(j))


def into(me, x, y, w, rows, dims, here, sends, after=None):
    free = 1 - dims[1][0]
    k, n = w.shape[dims[1][0]], w.shape[free]
    h = x.shape[1]
    first, count, groups = rows
    tall = count // groups // 2
    b = block_of(n, 3072 if free == 1 else 1536)

    def kernel(core_ref, x_ref, y_ref, w_ref, mine_ref, send_ref, held, *sems):
        one = pl.ds(first, count)
        low = core_ref[0] == 0
        w_from = w_ref if here else held

        def body(part):
            if free == 1:
                left, right = w_from[:h, part], w_from[h:, part]
            else:
                left, right = w_from[part, :h], w_from[part, h:]
            if free == 1:
                acc = dot(x_ref[one, :], left, NN) + dot(y_ref[one, :], right, NN)
            else:
                acc = (dot(left, x_ref[one, :], NT) + dot(right, y_ref[one, :], NT)).T
            for g in range(groups):
                at = 2 * g * tall
                lo, hi = acc[at : at + tall], acc[at + tall : at + 2 * tall]
                put = pl.ds(g * tall, tall)
                mine_ref[put, part] = jnp.where(low, lo, hi)
                send_ref[put, part] = jnp.where(low, hi, lo).astype(sends)

        stream(w_ref, held, None if here else sems[0], b, free, body)

    half = count // 2, n
    space = pltpu.VMEM if here else pltpu.HBM
    return call(
        kernel,
        [SMEM, VMEM, VMEM, VMEM if here else HBM],
        [VMEM, VMEM, VMEM],
        [jax.ShapeDtypeStruct(half, F32), jax.ShapeDtypeStruct(half, sends), pltpu.VMEM(w.shape, w.dtype)],
        [] if here else [pltpu.SemaphoreType.DMA((n // b,))],
        k * n,
        2 * k * n,
        me,
        x,
        y,
        pltpu.with_memory_space_constraint(w, space),
        aliases={3: 2} if here else {},
        after=after,
    )


def outof(me, own, other, w, dims, here, after):
    free = 1 - dims[1][0]
    k, n = w.shape[dims[1][0]], w.shape[free]
    half = own.shape[0]
    tall = max(2 * half, 128 if free == 1 else 0)
    b = block_of(n, 3072 if free == 1 else 1536)

    def kernel(core_ref, own_ref, other_ref, w_ref, keep_ref, send_ref, x_ref, *scratch):
        low = core_ref[0] == 0
        one, two = own_ref[...], other_ref[...]
        x_ref[:half, :] = jnp.where(low, one, two)
        x_ref[half : 2 * half, :] = jnp.where(low, two, one)
        if tall > 2 * half:
            x_ref[2 * half :, :] = jnp.zeros((tall - 2 * half, k), BF16)
        held, sems = scratch or (w_ref, None)

        def body(part):
            if free == 1:
                acc = dot(x_ref[...], held[:, part], NN)
            else:
                acc = dot(held[part, :], x_ref[...], NT).T
            keep_ref[:, part] = acc[:half]
            send_ref[:, part] = acc[half : 2 * half].astype(BF16)

        stream(w_ref, held, sems, b, free, body)

    scratch = [] if here else [pltpu.VMEM(w.shape, w.dtype), pltpu.SemaphoreType.DMA((n // b,))]
    return call(
        kernel,
        [SMEM, VMEM, VMEM, VMEM if here else HBM],
        [VMEM, VMEM],
        [jax.ShapeDtypeStruct((half, n), F32), jax.ShapeDtypeStruct((half, n), BF16)],
        [pltpu.VMEM((tall, k), BF16), *scratch],
        k * n,
        2 * k * n,
        me,
        own,
        other,
        pltpu.with_memory_space_constraint(w, pltpu.VMEM if here else pltpu.HBM),
        grant=6 if here else 26,
        after=after,
    )


def outer(jobs, after):
    blocks, olds = [], []
    for i, (x, _, old, first, rows) in enumerate(jobs):
        b = block_of(rows, 1024)
        blocks += [(i, first + j, b) for j in range(0, rows, b)]
        if old is not None:
            olds.append((i, pltpu.with_memory_space_constraint(old, pltpu.HBM)))
    tall = max(b for _, _, b in blocks)
    depth, width = jobs[0][1].shape
    count = len(jobs)
    wide = block_of(width, 512)
    columns = [[(c, wide) for c in range(0, width, wide)] for _ in blocks]

    def kernel(*refs):
        sides = refs[: 2 * count]
        outs = refs[2 * count + len(olds) : 3 * count + len(olds)]
        held, turned, sems = refs[3 * count + len(olds) :]
        copies = []
        for at, (i, row, b) in enumerate(blocks):
            part = pl.ds(row, b)
            turned[at, :b, :] = sides[2 * i][:, part].T
            for c, n in columns[at]:
                here = pl.ds(c, n)
                held[at, :b, here] = dot(turned[at, :b, :], sides[2 * i + 1][:, here], NN).astype(BF16)
                copies.append(
                    pltpu.make_async_copy(held.at[at, pl.ds(0, b), here], outs[i].at[part, here], sems.at[len(copies)])
                )
                copies[-1].start()
        for copy in copies:
            copy.wait()

    moved = sum(b for _, _, b in blocks) * width
    return call(
        kernel,
        [VMEM] * (2 * count) + [HBM] * len(olds),
        [HBM] * count,
        [pltpu.HBM((x.shape[1], width), BF16) for x, *_ in jobs],
        [
            pltpu.VMEM((len(blocks), tall, width), BF16),
            pltpu.VMEM((len(blocks), tall, depth), BF16),
            pltpu.SemaphoreType.DMA((sum(len(c) for c in columns),)),
        ],
        moved,
        2 * moved,
        *[side for x, y, *_ in jobs for side in (x, y)],
        *[old for _, old in olds],
        grant=20,
        aliases={2 * count + at: i for at, (i, _) in enumerate(olds)},
        after=after,
    )


def gather(left, right):
    all_bits = bits(lax.axis_size("row"))
    one = all_bits[::-1]
    two = all_bits[:1] + all_bits[:0:-1]
    order_one, order_two, ready = [0], [0], []
    tall = left.shape[1]
    for a, b in zip(one, two):
        ready.append(right)
        from_left, from_right = swap(left, "row", a), swap(right, "row", b)
        left = jnp.concatenate([left, from_left], axis=1)
        right = jnp.concatenate([right, from_right], axis=1)
        order_one += [j ^ a for j in order_one]
        order_two += [j ^ b for j in order_two]
    at = [order_two.index(j) * tall for j in order_one]
    right = jnp.concatenate([right[:, i : i + tall] for i in at], axis=1)
    return left, right, ready


def pair_sum(mine, send):
    return mine + swap(send, "col", 1).astype(F32)


def col_send(x):
    return lax.optimization_barrier(x.astype(BF16))


def col_sum(x, sent):
    for bit in bits(lax.axis_size("col"))[1:]:
        x = x + swap(sent, "col", bit).astype(F32)
        sent = x.astype(BF16)
    return x


def in_order(low, own, other):
    return jnp.concatenate([jnp.where(low, own, other), jnp.where(low, other, own)], axis=0)


def local(tokens, past_tokens, out_grad, w_in, w_out):
    me = lax.rem(lax.axis_index("col"), 2)
    x = jnp.stack([tokens, past_tokens, out_grad])
    x, me, low = lax.optimization_barrier((x, me.reshape(1), me == 0))
    width = x.shape[2]
    h = width // 2
    left, right, ready = gather(x[:, :, :h], x[:, :, h:])
    n = left.shape[1]
    half = n // 2
    left, right = left.reshape(3 * n, h), right.reshape(3 * n, h)
    w_in_here = load(w_in, None, 0, w_in.shape[0], ready[-1], 8)
    part = w_out.shape[0] // 2
    w_out_here = load(w_out, None, 0, part, ready[-3])
    w_out_here = load(w_out, w_out_here, part, part, ready[-2])
    mine, send, w_in_here = into(me, left, right, w_in_here, (0, 2 * n, 2), NN, True, BF16)
    pre = pair_sum(mine, send)
    sent = lax.optimization_barrier((pre[:half].astype(BF16), pre[half:].astype(BF16)))
    mine, send, w_out_here = into(me, left, right, w_out_here, (2 * n, n, 1), NT, True, F32, sent[0])
    back = pair_sum(mine, send)
    back_sent = col_send(back)
    past = col_sum(pre[half:], sent[1])
    act, slope = gelu_parts(past)
    act, slope = lax.optimization_barrier((act.astype(BF16), slope))
    now = col_sum(pre[:half], sent[0])
    hidden = gelu_parts(now)[0].astype(BF16)
    own, slope = lax.optimization_barrier((jnp.concatenate([hidden, act], axis=0), slope))
    other = swap(own, "col", 1)
    layer = outof(me, own[:half], other[:half], w_out_here, NN, True, back_sent)
    back = col_sum(back, back_sent)
    own_grad = (back * slope).astype(BF16)
    other_grad = swap(own_grad, "col", 1)
    inp = outof(me, own_grad, other_grad, w_in_here, NT, True, layer[1])
    past_all = jnp.concatenate([left[n : 2 * n], right[n : 2 * n]], axis=1)
    grad_all = jnp.concatenate([left[2 * n :], right[2 * n :]], axis=1)
    row_bits = bits(lax.axis_size("row"))
    sums = [keep + swap(send, "row", row_bits[0]).astype(F32) for (keep, send) in (layer, inp)]
    act_all, hidden_grad = in_order(low, own[half:], other[half:]), in_order(low, own_grad, other_grad)
    units = act_all.shape[1], past_all.shape[1]
    share = units[0] * 2 // 3 // 128 * 128, units[1] // 3 // 128 * 128
    (grad_w_out,) = outer([(act_all, grad_all, None, 0, share[0])], inp[1])
    res = jnp.concatenate(sums, axis=1)
    for i, bit in enumerate(row_bits[1:]):
        m = res.shape[0] // 2
        sent = lax.optimization_barrier(res[m:].astype(BF16))
        if i == 0:
            grad_w_out, grad_w_in = outer(
                [
                    (act_all, grad_all, grad_w_out, share[0], units[0] - share[0]),
                    (past_all, hidden_grad, None, 0, share[1]),
                ],
                sent,
            )
        elif i == 1:
            (grad_w_in,) = outer([(past_all, hidden_grad, grad_w_in, share[1], units[1] - share[1])], sent)
        res = res[:m] + swap(sent, "row", bit).astype(F32)
    res = res.astype(BF16)
    return (res[:, :width], res[:, width:], grad_w_in, grad_w_out)


def solution(mesh):
    in_specs = (P("row", "col"), P("row", "col"), P("row", "col"), P("col", "row"), P("row", "col"))
    out_specs = (P("row", "col"), P("row", "col"), P("col", "row"), P("row", "col"))

    return jax.shard_map(local, mesh=mesh, in_specs=in_specs, out_specs=out_specs, check_vma=False)
```

```python
import jax
import jax.numpy as jnp
from jax import lax
from jax.experimental import pallas as pl
from jax.experimental.pallas import tpu as pltpu
from jax.sharding import PartitionSpec as P


BF16, F32 = jnp.bfloat16, jnp.float32
MIB = 1 << 20
FLOPS = 128
NN, NT = ((1,), (0,)), ((1,), (1,))


def gelu_parts(pre):
    cdf = 0.5 * (1.0 + jax.scipy.special.erf(pre * 0.7071067811865476))
    slope = cdf + pre * jnp.exp(-0.5 * pre * pre) * 0.3989422804014327
    return (pre * cdf, slope)


def swap(x, axis, bit):
    n = lax.axis_size(axis)
    return lax.ppermute(x, axis, [(i, i ^ bit) for i in range(n)])


def bits(n):
    return [1 << k for k in range(n.bit_length() - 1)]


def block_of(n, most):
    return max(b for b in range(128, n + 1, 128) if n % b == 0 and b <= max(most, 128))


def dot(x, y, dims):
    return lax.dot_general(x, y, (dims, ((), ())), preferred_element_type=F32)


def call(kernel, in_specs, out_specs, out_shape, scratch, macs, moved, *args, grant=6, aliases={}, after=None):
    body = kernel
    if after is not None:
        in_specs, args = [*in_specs, pl.BlockSpec(memory_space=pl.ANY)], (*args, after)
        at = len(args) - 1

        def body(*refs):
            kernel(*refs[:at], *refs[at + 1 :])

    return pl.pallas_call(
        body,
        in_specs=in_specs,
        out_specs=out_specs,
        out_shape=out_shape,
        scratch_shapes=scratch,
        input_output_aliases=aliases,
        compiler_params=pltpu.CompilerParams(vmem_limit_bytes=grant * MIB),
        cost_estimate=pl.CostEstimate(flops=FLOPS * macs, bytes_accessed=moved, transcendentals=0),
    )(*args)


VMEM = pl.BlockSpec(memory_space=pltpu.VMEM)
SMEM = pl.BlockSpec(memory_space=pltpu.SMEM)
HBM = pl.BlockSpec(memory_space=pltpu.HBM)


def load(w, held, first, rows, after, parts=4):
    step = rows // parts
    old = [] if held is None else [pltpu.with_memory_space_constraint(held, pltpu.VMEM)]

    def kernel(w_ref, *refs):
        o_ref, sems = refs[-2:]
        copies = []
        for i in range(parts):
            part = pl.ds(first + i * step, step)
            copies.append(pltpu.make_async_copy(w_ref.at[part], o_ref.at[part], sems.at[i]))
            copies[-1].start()
        for copy in copies:
            copy.wait()

    return call(
        kernel,
        [HBM] + [VMEM] * len(old),
        VMEM,
        pltpu.VMEM(w.shape, w.dtype),
        [pltpu.SemaphoreType.DMA((parts,))],
        rows * w.shape[1],
        2 * rows * w.shape[1],
        pltpu.with_memory_space_constraint(w, pltpu.HBM),
        *old,
        grant=2,
        aliases={1: 0} if old else {},
        after=after,
    )


def stream(w_ref, held, sems, b, free, body, ahead=3):
    n = w_ref.shape[free] // b

    def part(j):
        return pl.ds(pl.multiple_of(j * b, b), b)

    def copy(j):
        at = (slice(None), part(j)) if free == 1 else (part(j), slice(None))
        return pltpu.make_async_copy(w_ref.at[at], held.at[at], sems.at[j])

    if sems is not None:
        for j in range(min(ahead, n)):
            copy(j).start()

    @pl.loop(0, n)
    def _(j):
        if sems is not None:
            copy(j).wait()

            @pl.when(j + ahead < n)
            def _():
                copy(j + ahead).start()

        body(part(j))


def into(me, x, y, w, rows, dims, here, sends, after=None):
    free = 1 - dims[1][0]
    k, n = w.shape[dims[1][0]], w.shape[free]
    h = x.shape[1]
    first, count, groups = rows
    tall = count // groups // 2
    b = block_of(n, 3072 if free == 1 else 1536)

    def kernel(core_ref, x_ref, y_ref, w_ref, mine_ref, send_ref, held, *sems):
        one = pl.ds(first, count)
        low = core_ref[0] == 0
        w_from = w_ref if here else held

        def body(part):
            if free == 1:
                left, right = w_from[:h, part], w_from[h:, part]
            else:
                left, right = w_from[part, :h], w_from[part, h:]
            if free == 1:
                acc = dot(x_ref[one, :], left, NN) + dot(y_ref[one, :], right, NN)
            else:
                acc = (dot(left, x_ref[one, :], NT) + dot(right, y_ref[one, :], NT)).T
            for g in range(groups):
                at = 2 * g * tall
                lo, hi = acc[at : at + tall], acc[at + tall : at + 2 * tall]
                put = pl.ds(g * tall, tall)
                mine_ref[put, part] = jnp.where(low, lo, hi)
                send_ref[put, part] = jnp.where(low, hi, lo).astype(sends)

        stream(w_ref, held, None if here else sems[0], b, free, body)

    half = count // 2, n
    space = pltpu.VMEM if here else pltpu.HBM
    return call(
        kernel,
        [SMEM, VMEM, VMEM, VMEM if here else HBM],
        [VMEM, VMEM, VMEM],
        [jax.ShapeDtypeStruct(half, F32), jax.ShapeDtypeStruct(half, sends), pltpu.VMEM(w.shape, w.dtype)],
        [] if here else [pltpu.SemaphoreType.DMA((n // b,))],
        k * n,
        2 * k * n,
        me,
        x,
        y,
        pltpu.with_memory_space_constraint(w, space),
        aliases={3: 2} if here else {},
        after=after,
    )


def outof(me, own, other, w, dims, here, after):
    free = 1 - dims[1][0]
    k, n = w.shape[dims[1][0]], w.shape[free]
    half = own.shape[0]
    tall = max(2 * half, 128 if free == 1 else 0)
    b = block_of(n, 3072 if free == 1 else 1536)

    def kernel(core_ref, own_ref, other_ref, w_ref, keep_ref, send_ref, x_ref, *scratch):
        low = core_ref[0] == 0
        one, two = own_ref[...], other_ref[...]
        x_ref[:half, :] = jnp.where(low, one, two)
        x_ref[half : 2 * half, :] = jnp.where(low, two, one)
        if tall > 2 * half:
            x_ref[2 * half :, :] = jnp.zeros((tall - 2 * half, k), BF16)
        held, sems = scratch or (w_ref, None)

        def body(part):
            if free == 1:
                acc = dot(x_ref[...], held[:, part], NN)
            else:
                acc = dot(held[part, :], x_ref[...], NT).T
            keep_ref[:, part] = acc[:half]
            send_ref[:, part] = acc[half : 2 * half].astype(BF16)

        stream(w_ref, held, sems, b, free, body)

    scratch = [] if here else [pltpu.VMEM(w.shape, w.dtype), pltpu.SemaphoreType.DMA((n // b,))]
    return call(
        kernel,
        [SMEM, VMEM, VMEM, VMEM if here else HBM],
        [VMEM, VMEM],
        [jax.ShapeDtypeStruct((half, n), F32), jax.ShapeDtypeStruct((half, n), BF16)],
        [pltpu.VMEM((tall, k), BF16), *scratch],
        k * n,
        2 * k * n,
        me,
        own,
        other,
        pltpu.with_memory_space_constraint(w, pltpu.VMEM if here else pltpu.HBM),
        grant=6 if here else 26,
        after=after,
    )


def outer(jobs, after):
    blocks, olds = [], []
    for i, (x, _, old, first, rows) in enumerate(jobs):
        b = block_of(rows, 1024)
        blocks += [(i, first + j, b) for j in range(0, rows, b)]
        if old is not None:
            olds.append((i, pltpu.with_memory_space_constraint(old, pltpu.HBM)))
    tall = max(b for _, _, b in blocks)
    depth, width = jobs[0][1].shape
    count = len(jobs)
    wide = block_of(width, 512)
    columns = [[(c, wide) for c in range(0, width, wide)] for _ in blocks]

    def kernel(*refs):
        sides = refs[: 2 * count]
        outs = refs[2 * count + len(olds) : 3 * count + len(olds)]
        held, turned, sems = refs[3 * count + len(olds) :]
        copies = []
        for at, (i, row, b) in enumerate(blocks):
            part = pl.ds(row, b)
            turned[at, :b, :] = sides[2 * i][:, part].T
            for c, n in columns[at]:
                here = pl.ds(c, n)
                held[at, :b, here] = dot(turned[at, :b, :], sides[2 * i + 1][:, here], NN).astype(BF16)
                copies.append(
                    pltpu.make_async_copy(held.at[at, pl.ds(0, b), here], outs[i].at[part, here], sems.at[len(copies)])
                )
                copies[-1].start()
        for copy in copies:
            copy.wait()

    moved = sum(b for _, _, b in blocks) * width
    return call(
        kernel,
        [VMEM] * (2 * count) + [HBM] * len(olds),
        [HBM] * count,
        [pltpu.HBM((x.shape[1], width), BF16) for x, *_ in jobs],
        [
            pltpu.VMEM((len(blocks), tall, width), BF16),
            pltpu.VMEM((len(blocks), tall, depth), BF16),
            pltpu.SemaphoreType.DMA((sum(len(c) for c in columns),)),
        ],
        moved,
        2 * moved,
        *[side for x, y, *_ in jobs for side in (x, y)],
        *[old for _, old in olds],
        grant=20,
        aliases={2 * count + at: i for at, (i, _) in enumerate(olds)},
        after=after,
    )


def gather(left, right):
    all_bits = bits(lax.axis_size("row"))
    one = all_bits[::-1]
    two = all_bits[:1] + all_bits[:0:-1]
    order_one, order_two, ready = [0], [0], []
    tall = left.shape[1]
    for a, b in zip(one, two):
        ready.append(right)
        from_left, from_right = swap(left, "row", a), swap(right, "row", b)
        left = jnp.concatenate([left, from_left], axis=1)
        right = jnp.concatenate([right, from_right], axis=1)
        order_one += [j ^ a for j in order_one]
        order_two += [j ^ b for j in order_two]
    at = [order_two.index(j) * tall for j in order_one]
    right = jnp.concatenate([right[:, i : i + tall] for i in at], axis=1)
    return left, right, ready


def pair_sum(mine, send):
    return mine + swap(send, "col", 1).astype(F32)


def col_send(x):
    return lax.optimization_barrier(x.astype(BF16))


def col_sum(x, sent):
    for bit in bits(lax.axis_size("col"))[1:]:
        x = x + swap(sent, "col", bit).astype(F32)
        sent = x.astype(BF16)
    return x


def in_order(low, own, other):
    return jnp.concatenate([jnp.where(low, own, other), jnp.where(low, other, own)], axis=0)


def local(tokens, past_tokens, out_grad, w_in, w_out):
    me = lax.rem(lax.axis_index("col"), 2)
    x = jnp.stack([tokens, past_tokens, out_grad])
    x, me, low = lax.optimization_barrier((x, me.reshape(1), me == 0))
    width = x.shape[2]
    h = width // 2
    left, right, ready = gather(x[:, :, :h], x[:, :, h:])
    n = left.shape[1]
    half = n // 2
    left, right = left.reshape(3 * n, h), right.reshape(3 * n, h)
    part = w_in.shape[0] // 4
    w_out_here = load(w_out, None, 0, part, ready[-3])
    w_out_here = load(w_out, w_out_here, part, 3 * part, ready[-2], 6)
    w_in_here = load(w_in, None, 0, w_in.shape[0], ready[-1], 8)
    mine, send, w_in_here = into(me, left, right, w_in_here, (0, 2 * n, 2), NN, True, BF16)
    pre = pair_sum(mine, send)
    sent = col_send(pre)
    mine, send, w_out_here = into(me, left, right, w_out_here, (2 * n, n, 1), NT, True, F32, sent)
    back = pair_sum(mine, send)
    back_sent = col_send(back)
    pre = col_sum(pre, sent)
    act, slope = gelu_parts(pre[half:])
    hidden = gelu_parts(pre[:half])[0].astype(BF16)
    act = act.astype(BF16)
    own, slope = lax.optimization_barrier((jnp.concatenate([hidden, act], axis=0), slope))
    other = swap(own, "col", 1)
    layer = outof(me, own[:half], other[:half], w_out_here, NN, True, back_sent)
    back = col_sum(back, back_sent)
    own_grad = (back * slope).astype(BF16)
    other_grad = swap(own_grad, "col", 1)
    inp = outof(me, own_grad, other_grad, w_in_here, NT, True, layer[1])
    past_all = jnp.concatenate([left[n : 2 * n], right[n : 2 * n]], axis=1)
    grad_all = jnp.concatenate([left[2 * n :], right[2 * n :]], axis=1)
    row_bits = bits(lax.axis_size("row"))
    sums = [keep + swap(send, "row", row_bits[0]).astype(F32) for (keep, send) in (layer, inp)]
    act_all, hidden_grad = in_order(low, own[half:], other[half:]), in_order(low, own_grad, other_grad)
    units = act_all.shape[1], past_all.shape[1]
    share = units[0] * 3 // 4 // 128 * 128, units[1] * 3 // 8 // 128 * 128
    (grad_w_out,) = outer([(act_all, grad_all, None, 0, share[0])], inp[1])
    res = jnp.concatenate(sums, axis=1)
    for i, bit in enumerate(row_bits[1:]):
        m = res.shape[0] // 2
        sent = lax.optimization_barrier(res[m:].astype(BF16))
        if i == 0:
            grad_w_out, grad_w_in = outer(
                [
                    (act_all, grad_all, grad_w_out, share[0], units[0] - share[0]),
                    (past_all, hidden_grad, None, 0, share[1]),
                ],
                sent,
            )
        elif i == 1:
            (grad_w_in,) = outer([(past_all, hidden_grad, grad_w_in, share[1], units[1] - share[1])], sent)
        res = res[:m] + swap(sent, "row", bit).astype(F32)
    res = res.astype(BF16)
    return (res[:, :width], res[:, width:], grad_w_in, grad_w_out)


def solution(mesh):
    in_specs = (P("row", "col"), P("row", "col"), P("row", "col"), P("col", "row"), P("row", "col"))
    out_specs = (P("row", "col"), P("row", "col"), P("col", "row"), P("row", "col"))

    return jax.shard_map(local, mesh=mesh, in_specs=in_specs, out_specs=out_specs, check_vma=False)
```
